32 devices in a mesh: row: 8 (over z, y), col: 4 (over x, core).
Axes of the slice: x: 2, y: 2, z: 4, core: 2. Of those that a mesh axis runs over, the one named last changes fastest.
Arguments:
- prior: float32 [2, 4096, 4096], P(None, 'row', 'col'), may hold values from 0.1 to 10
- first_tiles: bfloat16 [2, 32, 24, 128, 128], P(None, 'row'), may hold values from 0 to 1
- first_columns: int32 [2, 32, 24], P(None, 'row'), may hold values from 0 to 31, as said below
- first_counts: int32 [2, 32], P(None, 'row'), may hold values from 1 to 24, as said below
- second_network_tiles: bfloat16 [2, 32, 24, 128, 128], P(None, 'col'), may hold values from 0 to 1
- second_columns: int32 [2, 32, 24], P(None, 'col'), may hold values from 0 to 31, as said below
- second_counts: int32 [2, 32], P(None, 'col'), may hold values from 1 to 24, as said below
- sizes_first: int32 [2], replicated, may hold values from 2048 to 4096
- sizes_second: int32 [2], replicated, may hold values from 2048 to 4096
Outputs:
- similarity: float32 [2, 4096, 4096], P(None, 'row', 'col')
The draws below stay inside these ranges and needn't reach their ends.
Inputs may be any that keep to these rules, and one draw needn't show every extreme that they name: `first_columns`: within a tile row the 24 slots name distinct tile columns. Only the first first_counts[p, i] slots of tile row i are live; in every pair some tile row has all 24 live. `second_columns`: within a tile row the 24 slots name distinct tile columns. Only the first second_counts[p, i] slots of tile row i are live; in every pair some tile row has all 24 live.
All inputs are finite; a program needn't handle non-finite values.
Results may differ from the reference program's by a relative error of at most 0.00035.
Values may be sent and summed in bfloat16 or wider, within the bound.
A program may use at most 128 MiB of HBM per device.

```python
import math
import jax
import jax.numpy as jnp
from jax import lax

TILE = 128
N = 4096
NT = 32
SLOTS = 24
PAIRS = 2
ITERS = 2


def tile_columns(key):
    subkeys = jax.random.split(key, PAIRS * NT)
    shuffled = jax.vmap(lambda single_network: jax.random.permutation(single_network, NT))(subkeys)
    return shuffled[:, :SLOTS].reshape(PAIRS, NT, SLOTS).astype(jnp.int32)


def live_counts(key):
    counts = jax.random.randint(key, (PAIRS, NT), 1, SLOTS + 1)
    chosen = jax.random.randint(jax.random.fold_in(key, 1), (PAIRS,), 0, NT)
    positions = jnp.arange(NT)[None, :]
    return jnp.where(positions == chosen[:, None], SLOTS, counts).astype(jnp.int32)


def sparse_tiles(key):
    total = PAIRS * NT * SLOTS
    subkeys = jax.random.split(jax.random.fold_in(key, 1), total)
    matching = jax.vmap(lambda single_network: jax.random.permutation(single_network, TILE))(subkeys)
    on_match = matching[:, :, None] == jnp.arange(TILE)[None, None, :]
    extra = jax.random.randint(jax.random.fold_in(key, 2), (total, TILE, TILE), 0, TILE) == 0
    edges = on_match | extra
    weights = jnp.exp(jax.random.uniform(jax.random.fold_in(key, 3), (total, TILE, TILE), jnp.float32, math.log(0.05), 0.0))
    tiles = jnp.where(edges, weights, jnp.float32(0.0))
    return tiles.reshape(PAIRS, NT, SLOTS, TILE, TILE).astype(jnp.bfloat16)


def draw_first_tiles(key, part):
    return sparse_tiles(jax.random.fold_in(key, 21))


def draw_second_network_tiles(key, part):
    return sparse_tiles(jax.random.fold_in(key, 22))


def draw_first_columns(key, part):
    return tile_columns(jax.random.fold_in(key, 11))


def draw_second_columns(key, part):
    return tile_columns(jax.random.fold_in(key, 12))


def draw_first_counts(key, part):
    return live_counts(jax.random.fold_in(key, 13))


def draw_second_counts(key, part):
    return live_counts(jax.random.fold_in(key, 14))


def block_scale(own_key, dims, shards, smallest, largest):
    factor_of, own = 1.0, jax.random.fold_in(own_key, 6)
    for dim, parts in shards:
        draws = jnp.exp(jax.random.uniform(jax.random.fold_in(own, dim), (parts,), jnp.float32, smallest / len(shards), largest / len(shards)))
        factor_of = factor_of * jnp.repeat(draws, dims[dim] // parts).reshape([-1 if axis == dim else 1 for axis in range(len(dims))])
    return factor_of


def setup_inputs(seed: int = 0) -> dict:
    keys = jax.random.split(jax.random.key(seed), 10)
    return {
        "prior": jnp.clip(jnp.exp(math.log(10.0) - 4.6051702 * jax.random.uniform(keys[0], (PAIRS, N, N), jnp.float32) ** block_scale(keys[0], (PAIRS, N, N), ((1, 8), (2, 4)), -0.2, 0.2)), 0.1, 10.0),
        "first_tiles": draw_first_tiles(jax.random.fold_in(keys[9], 71), 0),
        "first_columns": draw_first_columns(jax.random.fold_in(keys[9], 71), 0),
        "first_counts": draw_first_counts(jax.random.fold_in(keys[9], 71), 0),
        "second_network_tiles": draw_second_network_tiles(jax.random.fold_in(keys[9], 71), 0),
        "second_columns": draw_second_columns(jax.random.fold_in(keys[9], 71), 0),
        "second_counts": draw_second_counts(jax.random.fold_in(keys[9], 71), 0),
        "sizes_first": jax.random.randint(keys[7], (PAIRS,), N // 2, N + 1).astype(jnp.int32),
        "sizes_second": jax.random.randint(keys[8], (PAIRS,), N // 2, N + 1).astype(jnp.int32),
    }


propagation = 0.7

def first_product(tiles, columns, counts, panel):
    blocks = panel.reshape(NT, TILE, panel.shape[1])
    in_use = jnp.arange(SLOTS)[None, :] < counts[:, None]

    def one_row(operands):
        row_block_tiles, row_columns, row_use = operands
        selected_entries = blocks[row_columns].astype(jnp.float32)
        masked_entries = jnp.where(row_use[:, None, None], row_block_tiles.astype(jnp.float32), jnp.float32(0.0))
        return jnp.einsum('sab,sbc->ac', masked_entries, selected_entries)
    similarity_output = lax.map(one_row, (tiles, columns, in_use))
    return similarity_output.reshape(N, panel.shape[1])

def second_product(tiles, columns, counts, product):
    blocks = product.reshape(product.shape[0], NT, TILE)
    in_use = jnp.arange(SLOTS)[None, :] < counts[:, None]

    def one_row(operands):
        row_block_tiles, row_columns, row_use = operands
        selected_entries = blocks[:, row_columns].astype(jnp.float32)
        masked_entries = jnp.where(row_use[:, None, None], row_block_tiles.astype(jnp.float32), jnp.float32(0.0))
        return jnp.einsum('rsk,sck->rc', selected_entries, masked_entries)
    similarity_output = lax.map(one_row, (tiles, columns, in_use))
    return jnp.transpose(similarity_output, (1, 0, 2)).reshape(product.shape[0], N)

def reference(prior, first_tiles, first_columns, first_counts, second_network_tiles, second_columns, second_counts, sizes_first, sizes_second):
    positions = jnp.arange(N)
    results = []
    for pair_index in range(PAIRS):
        active = (positions < sizes_first[pair_index])[:, None] & (positions < sizes_second[pair_index])[None, :]
        initial = jnp.where(active, prior[pair_index], jnp.float32(0.0))
        entries = sizes_first[pair_index].astype(jnp.float32) * sizes_second[pair_index].astype(jnp.float32)
        current = initial
        for iteration in range(ITERS):
            panel = current.astype(jnp.bfloat16)
            product = first_product(first_tiles[pair_index], first_columns[pair_index], first_counts[pair_index], panel).astype(jnp.bfloat16)
            image = jnp.where(active, second_product(second_network_tiles[pair_index], second_columns[pair_index], second_counts[pair_index], product), jnp.float32(0.0))
            divisor = jnp.sqrt(jnp.sum(image * image) / entries + 1e-06)
            current = propagation * image / divisor + (1.0 - propagation) * initial
        results.append(current)
    return jnp.stack(results)
```

```python
import functools

import jax
import jax.numpy as jnp
from jax import lax
from jax.experimental import pallas as pl
from jax.experimental.pallas import tpu as pltpu
from jax.sharding import PartitionSpec as P

ITERS = 2
CHUNKS = 4

propagation = 0.7


def expand_kernel(positions_ref, live_ref, tiles_ref, dense_ref):
    tile_row = pl.program_id(0)
    slots, tile = tiles_ref.shape[1], tiles_ref.shape[2]
    per_group = dense_ref.shape[2] // tile
    dense_ref[...] = jnp.zeros_like(dense_ref)

    def place(slot, carry):
        position = positions_ref[tile_row, slot]
        group = position // per_group
        start = pl.multiple_of((position - group * per_group) * tile, tile)
        live = slot < live_ref[tile_row]
        entries = tiles_ref[0, slot]
        dense_ref[group, :, pl.ds(start, tile)] = jnp.where(live, entries, jnp.zeros_like(entries))
        return carry

    lax.fori_loop(0, slots, place, 0, unroll=True)


def expand(tiles, positions, counts, groups, width):
    rows, slots, tile, _ = tiles.shape
    return pl.pallas_call(
        expand_kernel,
        out_shape=jax.ShapeDtypeStruct((groups, rows * tile, width // groups), tiles.dtype),
        grid_spec=pltpu.PrefetchScalarGridSpec(
            num_scalar_prefetch=2,
            grid=(rows,),
            in_specs=[pl.BlockSpec((1, slots, tile, tile), lambda i, *_: (i, 0, 0, 0))],
            out_specs=pl.BlockSpec((groups, tile, width // groups), lambda i, *_: (0, i, 0)),
        ),
        cost_estimate=pl.CostEstimate(
            flops=0, bytes_accessed=2 * rows * tile * (slots * tile + width), transcendentals=0
        ),
        name="expand",
    )(positions, counts, tiles)


def shards(rows_total, cols_total, *args):
    (prior, first_tiles, first_columns, first_counts, second_tiles, second_columns,
     second_counts, sizes_first, sizes_second) = args
    pairs, height, width = prior.shape
    assert pairs == 2 and rows_total % 2 == 0 and cols_total % 2 == 0
    tile = first_tiles.shape[-1]
    nodes_first, nodes_second = height * rows_total, width * cols_total
    ring, across = rows_total // 2, cols_total // 2
    chunks = CHUNKS
    while width // chunks < 2 * tile and chunks > 1:
        chunks //= 2
    piece = width // chunks

    row, col = lax.axis_index("row"), lax.axis_index("col")
    y, z = row % 2, row // 2
    core, x = col % 2, col // 2
    first_core = core == 0

    row_swap = [(i, i ^ 1) for i in range(rows_total)]
    col_swap = [(i, i ^ 1) for i in range(cols_total)]

    def along(array, steps):
        return lax.ppermute(array, "row", [((i + 2 * steps) % rows_total, i) for i in range(rows_total)])

    def swap_rows(array):
        return lax.ppermute(array, "row", row_swap)

    def swap_cols(array):
        return lax.ppermute(array, "col", col_swap)

    def mine(array):
        return jnp.where(first_core, array[0], array[1])

    def other(array):
        return jnp.where(first_core, array[1], array[0])

    size_first, size_second = mine(sizes_first), mine(sizes_second)
    row_ids = row * height + jnp.arange(height, dtype=jnp.int32)
    col_ids = jnp.arange(width, dtype=jnp.int32)
    in_rows = (row_ids < size_first)[:, None]
    active_own = in_rows & (col * width + col_ids < size_second)[None, :]
    active_other = in_rows & ((col ^ 1) * width + col_ids < size_second)[None, :]
    prior_other = swap_cols(other(prior))
    initial_own = jnp.where(active_own, mine(prior), jnp.float32(0.0))
    initial_other = jnp.where(active_other, prior_other, jnp.float32(0.0))
    entries = size_first.astype(jnp.float32) * size_second.astype(jnp.float32)

    per_row = height // tile

    def first_places(columns):
        owner = columns // per_row
        step = (owner // 2 - z + ring) % ring
        return (step * 2 + ((owner % 2) ^ y)) * per_row + columns % per_row

    f_tiles, f_columns, f_counts = mine(first_tiles), mine(first_columns), mine(first_counts)
    a_own = expand(f_tiles, first_places(f_columns), f_counts, 1, nodes_first)[0]
    a_next = expand(
        swap_rows(f_tiles), first_places(swap_rows(f_columns)), swap_rows(f_counts), 1, nodes_first
    )[0]

    per_col = width // tile
    per_piece = per_col // chunks

    def second_places(columns):
        owner, inside = columns // per_col, columns % per_col
        step = (owner // 2 - x + across) % across
        block = ((inside // per_piece) * across + step) * 2 + ((owner % 2) ^ y)
        return block * per_piece + inside % per_piece

    b_own = expand(
        mine(second_tiles), second_places(mine(second_columns)), mine(second_counts), chunks, nodes_second
    )
    b_other = expand(
        swap_cols(other(second_tiles)),
        second_places(swap_cols(other(second_columns))),
        swap_cols(other(second_counts)),
        chunks,
        nodes_second,
    )

    keeps_own = y == core

    def gather_ring(block, forward):
        ahead = ring // 2 if forward else (ring - 1) // 2
        behind = ring - 1 - ahead
        blocks = {0: block}
        for step in range(1, max(ahead, behind) + 1):
            if step <= ahead:
                blocks[step] = along(blocks[step - 1], 1)
            if step <= behind:
                blocks[-step % ring] = along(blocks[(1 - step) % ring], -1)
        return jnp.concatenate([blocks[step] for step in range(ring)], axis=0)

    def dot(a, b):
        return lax.dot_general(a, b, (((1,), (0,)), ((), ())), preferred_element_type=jnp.float32)

    def dot_t(a, b):
        return lax.dot_general(a, b, (((1,), (1,)), ((), ())), preferred_element_type=jnp.float32)

    own, far = initial_own, initial_other
    for iteration in range(ITERS):
        panel_own, panel_far = own.astype(jnp.bfloat16), far.astype(jnp.bfloat16)
        image_own = image_far = None
        stacks = []
        for j in range(chunks):
            span = slice(j * piece, (j + 1) * piece)
            keep = jnp.where(keeps_own, panel_own[:, span], panel_far[:, span])
            send = jnp.where(keeps_own, panel_far[:, span], panel_own[:, span])
            block = jnp.concatenate([keep, swap_rows(send)], axis=0)
            stacks.append(gather_ring(block, j % 2 == 0))
        for j in range(chunks):
            product_next = dot(a_next, stacks[j]).astype(jnp.bfloat16)
            product_own = dot(a_own, stacks[j]).astype(jnp.bfloat16)
            product = jnp.concatenate([product_own, swap_rows(product_next)], axis=1)
            parts = [product]
            for step in range(1, across):
                parts.append(
                    lax.ppermute(
                        product, "col", [((i + 2 * step) % cols_total, i) for i in range(cols_total)]
                    )
                )
            gathered = jnp.concatenate(parts, axis=1)
            term_own, term_far = dot_t(gathered, b_own[j]), dot_t(gathered, b_other[j])
            image_own = term_own if image_own is None else image_own + term_own
            image_far = term_far if image_far is None else image_far + term_far
        image_own = jnp.where(active_own, image_own, jnp.float32(0.0))
        image_far = jnp.where(active_other, image_far, jnp.float32(0.0))
        local = jnp.sum(image_own * image_own) + jnp.sum(image_far * image_far)
        sums = lax.psum(jnp.where(jnp.arange(2) == core, local, jnp.float32(0.0)), ("row", "col"))
        divisor = jnp.sqrt(mine(sums) / entries + 1e-06)
        own = propagation * image_own / divisor + (1.0 - propagation) * initial_own
        far = propagation * image_far / divisor + (1.0 - propagation) * initial_other
    arrived = swap_cols(far)
    return jnp.stack([jnp.where(first_core, own, arrived), jnp.where(first_core, arrived, own)])


def solution(mesh):
    in_specs = (
        P(None, "row", "col"),
        P(None, "row", None, None, None),
        P(None, "row", None),
        P(None, "row"),
        P(None, "col", None, None, None),
        P(None, "col", None),
        P(None, "col"),
        P(),
        P(),
    )
    out_specs = P(None, "row", "col")
    local = functools.partial(shards, mesh.shape["row"], mesh.shape["col"])
    return jax.shard_map(local, mesh=mesh, in_specs=in_specs, out_specs=out_specs, check_vma=False)
```

```python
import jax
import jax.numpy as jnp
from jax import lax
from jax.experimental import pallas as pl
from jax.experimental.pallas import tpu as pltpu
from jax.sharding import PartitionSpec as P


ITERS = 2
CHUNKS = 4

propagation = 0.7


def expand_kernel(where_ref, positions_ref, live_ref, tiles_ref, dense_ref):
    tile_row = pl.program_id(0)
    slots, tile = tiles_ref.shape[2], tiles_ref.shape[3]
    per_group = dense_ref.shape[2] // tile
    dense_ref[...] = jnp.zeros_like(dense_ref)

    def place(slot, carry):
        position = positions_ref[tile_row, slot]
        group = position // per_group
        start = pl.multiple_of((position - group * per_group) * tile, tile)
        live = slot < live_ref[tile_row]
        entries = tiles_ref[0, 0, slot]
        dense_ref[group, :, pl.ds(start, tile)] = jnp.where(live, entries, jnp.zeros_like(entries))
        return carry

    lax.fori_loop(0, slots, place, 0, unroll=True)


def expand(tiles, pair, shift, positions, counts, groups, width):
    _, rows, slots, tile, _ = tiles.shape
    where = jnp.stack([pair, shift]).astype(jnp.int32)
    return pl.pallas_call(
        expand_kernel,
        out_shape=jax.ShapeDtypeStruct((groups, rows * tile, width // groups), tiles.dtype),
        grid_spec=pltpu.PrefetchScalarGridSpec(
            num_scalar_prefetch=3,
            grid=(rows,),
            in_specs=[
                pl.BlockSpec((1, 1, slots, tile, tile), lambda i, w, *_: (w[0], i, 0, 0, 0))
            ],
            out_specs=pl.BlockSpec(
                (groups, tile, width // groups),
                lambda i, w, *_: (0, lax.rem(i + w[1], rows), 0),
            ),
        ),
        cost_estimate=pl.CostEstimate(
            flops=0, bytes_accessed=2 * rows * tile * (slots * tile + width), transcendentals=0
        ),
        name="expand",
    )(where, positions, counts, tiles)


def ring_steps(ring, forward):
    ahead = ring // 2 if forward else (ring - 1) // 2
    return ahead, ring - 1 - ahead


def shards(rows_total, cols_total, *args):
    (prior, first_tiles, first_columns, first_counts, second_tiles, second_columns,
     second_counts, sizes_first, sizes_second) = args
    pairs, height, width = prior.shape
    assert pairs == 2 and rows_total % 2 == 0 and cols_total % 2 == 0
    tile = first_tiles.shape[-1]
    nodes_first, nodes_second = height * rows_total, width * cols_total
    ring, across = rows_total // 2, cols_total // 2
    chunks = CHUNKS
    while width // chunks < 2 * tile and chunks > 1:
        chunks //= 2
    piece = width // chunks

    row, col = lax.axis_index("row"), lax.axis_index("col")
    y, z = row % 2, row // 2
    core, x = col % 2, col // 2
    first_core = core == 0

    row_swap = [(i, i ^ 1) for i in range(rows_total)]
    col_swap = [(i, i ^ 1) for i in range(cols_total)]

    def along(array, steps):
        return lax.ppermute(array, "row", [((i + 2 * steps) % rows_total, i) for i in range(rows_total)])

    def swap_rows(array):
        return lax.ppermute(array, "row", row_swap)

    def swap_cols(array):
        return lax.ppermute(array, "col", col_swap)

    def mine(array):
        return jnp.where(first_core, array[0], array[1])

    def other(array):
        return jnp.where(first_core, array[1], array[0])

    size_first, size_second = mine(sizes_first), mine(sizes_second)
    row_ids = row * height + jnp.arange(height, dtype=jnp.int32)
    col_ids = jnp.arange(width, dtype=jnp.int32)
    in_rows = (row_ids < size_first)[:, None]
    active_own = in_rows & (col * width + col_ids < size_second)[None, :]
    active_other = in_rows & ((col ^ 1) * width + col_ids < size_second)[None, :]
    prior_other = swap_cols(lax.dynamic_index_in_dim(prior, 1 - core, 0, keepdims=False))
    initial_own = jnp.where(active_own, mine(prior), jnp.float32(0.0))
    initial_other = jnp.where(active_other, prior_other, jnp.float32(0.0))
    entries = size_first.astype(jnp.float32) * size_second.astype(jnp.float32)

    per_row = height // tile

    def first_places(columns):
        owner = columns // per_row
        step = (owner // 2 - z + ring) % ring
        return (step * 2 + ((owner % 2) ^ y)) * per_row + columns % per_row

    f_columns, f_counts = mine(first_columns), mine(first_counts)
    zero = jnp.int32(0)
    a_own = expand(first_tiles, core, zero, first_places(f_columns), f_counts, 1, nodes_first)[0]
    next_columns, next_counts = swap_rows(f_columns), swap_rows(f_counts)
    if across % 2 == 0 and per_row % 2 == 0:
        half = per_row // 2
        shift = (x % 2) * half
        start = (core, shift, zero, zero, zero)
        part = lax.dynamic_slice(first_tiles, start, (1, half) + first_tiles.shape[2:])
        part = swap_rows(part)
        shared = lax.ppermute(part, "col", [(i, i ^ 2) for i in range(cols_total)])
        next_tiles = jnp.concatenate([part, shared], axis=1)
        source_rows = (jnp.arange(per_row) + shift) % per_row
        next_columns, next_counts = next_columns[source_rows], next_counts[source_rows]
    else:
        shift = zero
        next_tiles = swap_rows(mine(first_tiles)[None])
    a_next = expand(next_tiles, zero, shift, first_places(next_columns), next_counts, 1, nodes_first)[0]

    per_col = width // tile
    per_piece = per_col // chunks

    def second_places(columns):
        owner, inside = columns // per_col, columns % per_col
        step = (owner // 2 - x + across) % across
        block = ((inside // per_piece) * across + step) * 2 + ((owner % 2) ^ y)
        return block * per_piece + inside % per_piece

    b_own = expand(
        second_tiles, core, zero, second_places(mine(second_columns)), mine(second_counts), chunks,
        nodes_second,
    )
    picked = lax.dynamic_slice_in_dim(second_tiles, 1 - core, 1, axis=0)
    picked = swap_cols(picked)
    b_other = expand(
        picked, zero, zero, second_places(swap_cols(other(second_columns))),
        swap_cols(other(second_counts)), chunks, nodes_second,
    )

    keeps_own = y == core

    def gather_ring(block, forward):
        ahead, behind = ring_steps(ring, forward)
        blocks = {0: block}
        for step in range(1, max(ahead, behind) + 1):
            if step <= ahead:
                blocks[step] = along(blocks[step - 1], 1)
            if step <= behind:
                blocks[-step % ring] = along(blocks[(1 - step) % ring], -1)
        return jnp.concatenate([blocks[step] for step in range(ring)], axis=0)

    def total(value):
        if rows_total & (rows_total - 1) or cols_total & (cols_total - 1):
            both = jnp.where(jnp.arange(2) == core, value, jnp.float32(0.0))
            return mine(lax.psum(both, ("row", "col")))
        value = value[None]
        for axis, size, step in (("row", rows_total, 1), ("col", cols_total, 2)):
            while step < size:
                value = value + lax.ppermute(value, axis, [(i, i ^ step) for i in range(size)])
                step *= 2
        return value[0]

    def dot(a, b):
        return lax.dot_general(a, b, (((1,), (0,)), ((), ())), preferred_element_type=jnp.float32)

    def dot_t(a, b):
        return lax.dot_general(a, b, (((1,), (1,)), ((), ())), preferred_element_type=jnp.float32)

    own, far = initial_own, initial_other
    for _ in range(ITERS):
        panel_own, panel_far = own.astype(jnp.bfloat16), far.astype(jnp.bfloat16)
        image_own = image_far = None
        stacks = []
        for j in range(chunks):
            span = slice(j * piece, (j + 1) * piece)
            keep = jnp.where(keeps_own, panel_own[:, span], panel_far[:, span])
            send = jnp.where(keeps_own, panel_far[:, span], panel_own[:, span])
            received = swap_rows(send)
            block = jnp.concatenate([keep, received], axis=0)
            stacks.append(gather_ring(block, j % 2 == 0))
        for j in range(chunks):
            product_next = dot(a_next, stacks[j]).astype(jnp.bfloat16)
            product_own = dot(a_own, stacks[j]).astype(jnp.bfloat16)
            returned = swap_rows(product_next)
            product = jnp.concatenate([product_own, returned], axis=1)
            parts = [product]
            for step in range(1, across):
                parts.append(
                    lax.ppermute(
                        product, "col", [((i + 2 * step) % cols_total, i) for i in range(cols_total)]
                    )
                )
            gathered = jnp.concatenate(parts, axis=1)
            term_own, term_far = dot_t(gathered, b_own[j]), dot_t(gathered, b_other[j])
            image_own = term_own if image_own is None else image_own + term_own
            image_far = term_far if image_far is None else image_far + term_far
        image_own = jnp.where(active_own, image_own, jnp.float32(0.0))
        image_far = jnp.where(active_other, image_far, jnp.float32(0.0))
        local = jnp.sum(image_own * image_own) + jnp.sum(image_far * image_far)
        divisor = jnp.sqrt(total(local) / entries + 1e-06)
        own = propagation * image_own / divisor + (1.0 - propagation) * initial_own
        far = propagation * image_far / divisor + (1.0 - propagation) * initial_other
    arrived = swap_cols(far)
    return jnp.stack([jnp.where(first_core, own, arrived), jnp.where(first_core, arrived, own)])


def solution(mesh):
    in_specs = (
        P(None, "row", "col"),
        P(None, "row", None, None, None),
        P(None, "row", None),
        P(None, "row"),
        P(None, "col", None, None, None),
        P(None, "col", None),
        P(None, "col"),
        P(),
        P(),
    )
    out_specs = P(None, "row", "col")

    def local(*args):
        return shards(mesh.shape["row"], mesh.shape["col"], *args)

    return jax.shard_map(local, mesh=mesh, in_specs=in_specs, out_specs=out_specs, check_vma=False)
```
